32 devices in a mesh: section: 4 (over y, x), dp: 8 (over z, core).
Axes of the slice: x: 2, y: 2, z: 4, core: 2. Of those that a mesh axis runs over, the one named last changes fastest.
Arguments:
- inputs: bfloat16 [4, 2, 512, 4096], P('section', None, 'dp'), may hold values from -6 to 6
- cotangent: bfloat16 [2, 512, 4096], P(None, 'dp'), may hold values from -6 to 6
- norm_gain: bfloat16 [4, 4096], P('section', 'dp'), may hold values from 0.5 to 1.5
- key_weight: bfloat16 [4, 4096, 512], P('section', 'dp'), may hold values from -0.09375 to 0.09375
- value_weight: bfloat16 [4, 4096, 512], P('section', 'dp'), may hold values from -0.09375 to 0.09375
- plan: int32 [4, 2], P('section'), may hold values from 0 to 1, each once within a row
Outputs:
- grad_inputs: bfloat16 [4, 2, 512, 4096], P('section', None, 'dp')
- key_weight_grad: float32 [4, 4096, 512], P('section', 'dp')
- value_weight_grad: float32 [4, 4096, 512], P('section', 'dp')
- gain_grad: float32 [4, 4096], P('section', 'dp')
The draws below stay inside these ranges and needn't reach their ends.
Inputs may be any that keep to these rules, and one draw needn't show every extreme that they name: Each row of plan lists every micro-batch once.
All inputs are finite; a program needn't handle non-finite values.
Results may differ from the reference program's by a relative error of at most 0.03.
Values may be sent and summed in bfloat16 or wider, within the bound.
A program may use at most 128 MiB of HBM per device.

```python
import math
import jax
import jax.numpy as jnp
from jax import lax

D = 4096
HEADS = 32
KV_HEADS = 4
HEAD_DIM = 128
KV = 512
GROUP = 8
MB = 2
TOK_DEV = 64
TOKENS = 512
N_SECTION = 4
N_DP = 8


def strengthened(drawn, stream_key, source, target, blocks, factor):
    def block_of(position):
        return (jnp.arange(drawn.shape[position]) // (drawn.shape[position] // blocks)).reshape((-1,) + (1,) * (drawn.ndim - 1 - position))

    near = jax.random.permutation(stream_key, blocks)[block_of(target)]
    second = (block_of(target) + blocks // 2) % blocks
    return jnp.where((block_of(source) == near) | (block_of(source) == second), factor * drawn, drawn)


def level_of(key, shape, cuts, low, largest):
    level = 1.0
    for position, blocks in cuts:
        heights = jax.random.uniform(jax.random.fold_in(jax.random.fold_in(key, 6), position), (blocks,), jnp.float32, low / len(cuts), largest / len(cuts))
        level = level * jnp.repeat(jnp.exp(heights), shape[position] // blocks).reshape((-1,) + (1,) * (len(shape) - 1 - position))
    return level


def normal_values(stream_key, dims, scale, limit, split=(), held_as=jnp.bfloat16):
    entries = scale * jax.random.normal(stream_key, dims, jnp.float32)
    if split:
        entries = entries * level_of(stream_key, dims, split, -0.22, 0.18)
    return jnp.clip(entries, -limit, limit).astype(held_as)


def noise_with(stream_key, extent, spread, most, split, heavy, kind=jnp.bfloat16):
    result = spread * jax.random.normal(stream_key, extent, jnp.float32)
    if split:
        result = result * level_of(stream_key, extent, split, -0.22, 0.18)
    return jnp.clip(strengthened(result, jax.random.fold_in(stream_key, 3), *heavy), -most, most).astype(kind)


def setup_inputs(seed: int = 0) -> dict:
    splits = jax.random.split(jax.random.key(seed), 7)
    return {
        "inputs": noise_with(splits[0], (N_SECTION, MB, TOKENS, D), 1.0, 6.0, ((0, 4), (2, 8)), (2, 3, 8, 2.0)),
        "cotangent": normal_values(splits[1], (MB, TOKENS, D), 1.0, 6.0, ((1, 8),)),
        "norm_gain": jnp.clip(1.0 + 0.1 * jax.random.normal(splits[2], (N_SECTION, D), jnp.float32), 0.5, 1.5).astype(jnp.bfloat16),
        "key_weight": normal_values(splits[3], (N_SECTION, D, KV), D ** -0.5, 0.09375, ((0, 4), (1, 8))),
        "value_weight": normal_values(splits[4], (N_SECTION, D, KV), D ** -0.5, 0.09375, ((0, 4), (1, 8))),
        "plan": jax.vmap(lambda own: jax.random.permutation(own, MB))(jax.random.split(splits[5], N_SECTION)).reshape((N_SECTION, MB)).astype(jnp.int32),
    }


eps = 1e-05
rope_base = 500000.0

def rope_tables(length, head_dim):
    half_dim = head_dim // 2
    frequency = rope_base ** (-(jnp.arange(half_dim, dtype=jnp.float32) * 2.0 / head_dim))
    angles = jnp.arange(length, dtype=jnp.float32)[:, None] * frequency[None, :]
    cosine = jnp.concatenate([jnp.cos(angles), jnp.cos(angles)], axis=-1)
    sine_tab = jnp.concatenate([jnp.sin(angles), jnp.sin(angles)], axis=-1)
    return (cosine[:, None, :], sine_tab[:, None, :])

def turned(values):
    half_dim = values.shape[-1] // 2
    return jnp.concatenate([-values[..., half_dim:], values[..., :half_dim]], axis=-1)

def rotate(values, cosine, sine_tab):
    return values * cosine + turned(values) * sine_tab

def unrotate(values, cosine, sine_tab):
    return values * cosine - turned(values) * sine_tab

def forward(x_rows, gain, w_key, w_value):
    batch_count = x_rows.shape[0]
    length = x_rows.shape[1]
    score_scale = 1.0 / math.sqrt(HEAD_DIM)
    widened = x_rows.astype(jnp.float32)
    inv_rms = lax.rsqrt(lax.optimization_barrier(jnp.mean(widened * widened, axis=-1, keepdims=True)) + eps)
    gain_full = gain.astype(jnp.float32)
    normed = (widened * inv_rms * gain_full).astype(jnp.bfloat16)
    flat_normed = normed.reshape(batch_count * length, D)
    key_pre = jnp.dot(flat_normed, w_key, preferred_element_type=jnp.float32).reshape(batch_count, length, KV_HEADS, HEAD_DIM)
    value_heads = jnp.dot(flat_normed, w_value, preferred_element_type=jnp.float32).astype(jnp.bfloat16).reshape(batch_count, length, KV_HEADS, HEAD_DIM)
    cosine, sine_tab = rope_tables(length, HEAD_DIM)
    key_rot = rotate(key_pre, cosine, sine_tab).astype(jnp.bfloat16)
    query_rot = rotate(normed.astype(jnp.float32).reshape(batch_count, length, HEADS, HEAD_DIM), cosine, sine_tab).astype(jnp.bfloat16)
    query_rot = query_rot.reshape(batch_count, length, KV_HEADS, GROUP, HEAD_DIM)
    scores = jnp.einsum('blkgd,bmkd->bkglm', query_rot.astype(jnp.float32), key_rot.astype(jnp.float32)) * score_scale
    causal = jnp.arange(length)[:, None] >= jnp.arange(length)[None, :]
    raised = jnp.where(causal, jnp.exp(scores), 0.0)
    attn_prob = raised / lax.optimization_barrier(jnp.sum(raised, axis=-1, keepdims=True))
    prob_low = attn_prob.astype(jnp.bfloat16)
    return (widened, inv_rms, normed, query_rot, key_rot, value_heads, attn_prob, prob_low)

def backward(upper_grad, widened, inv_rms, normed, query_rot, key_rot, value_heads, attn_prob, prob_low, gain, w_key, w_value):
    batch_count = upper_grad.shape[0]
    length = upper_grad.shape[1]
    score_scale = 1.0 / math.sqrt(HEAD_DIM)
    grad_heads = upper_grad.astype(jnp.float32).reshape(batch_count, length, KV_HEADS, GROUP, HEAD_DIM)
    grad_prob = jnp.einsum('blkgd,bmkd->bkglm', grad_heads, value_heads.astype(jnp.float32))
    grad_value = jnp.einsum('bkglm,blkgd->bmkd', prob_low.astype(jnp.float32), grad_heads).astype(jnp.bfloat16)
    row_dot = lax.optimization_barrier(jnp.sum(attn_prob * grad_prob, axis=-1, keepdims=True))
    grad_score = (attn_prob * (grad_prob - row_dot) * score_scale).astype(jnp.bfloat16)
    grad_query = jnp.einsum('bkglm,bmkd->blkgd', grad_score.astype(jnp.float32), key_rot.astype(jnp.float32))
    grad_key = jnp.einsum('bkglm,blkgd->bmkd', grad_score.astype(jnp.float32), query_rot.astype(jnp.float32))
    cosine, sine_tab = rope_tables(length, HEAD_DIM)
    query_back = unrotate(grad_query.reshape(batch_count, length, HEADS, HEAD_DIM), cosine, sine_tab).reshape(batch_count, length, D)
    key_back = unrotate(grad_key, cosine, sine_tab).astype(jnp.bfloat16).reshape(batch_count * length, KV)
    value_flat = grad_value.reshape(batch_count * length, KV)
    projected_back = jnp.dot(key_back, w_key.T, preferred_element_type=jnp.float32) + jnp.dot(value_flat, w_value.T, preferred_element_type=jnp.float32)
    grad_normed = query_back + projected_back.reshape(batch_count, length, D)
    gain_full = gain.astype(jnp.float32)
    gain_term = grad_normed * widened * inv_rms
    projected = lax.optimization_barrier(jnp.mean(gain_term * gain_full, axis=-1, keepdims=True))
    lower_grad = upper_grad.astype(jnp.float32) + inv_rms * gain_full * grad_normed - widened * inv_rms * inv_rms * projected
    return (lower_grad.astype(jnp.bfloat16), key_back, value_flat, gain_term)

def regroup(array):
    return array.reshape(MB, N_DP, TOK_DEV, -1).transpose(1, 0, 2, 3).reshape(N_DP, MB * TOK_DEV, -1)

def add_group(totals, pieces):
    normed, key_back, value_flat, gain_term = pieces
    sum_key = jnp.dot(normed.T, key_back, preferred_element_type=jnp.float32)
    sum_value = jnp.dot(normed.T, value_flat, preferred_element_type=jnp.float32)
    sum_gain = lax.optimization_barrier(jnp.sum(gain_term, axis=0))
    rounded_key = lax.optimization_barrier(sum_key.astype(jnp.bfloat16)).astype(jnp.float32)
    rounded_value = lax.optimization_barrier(sum_value.astype(jnp.bfloat16)).astype(jnp.float32)
    rounded_gain = lax.optimization_barrier(sum_gain.astype(jnp.bfloat16)).astype(jnp.float32)
    return ((totals[0] + rounded_key, totals[1] + rounded_value, totals[2] + rounded_gain), None)

def reference(inputs, cotangent, norm_gain, key_weight, value_weight, plan):
    upper_grad = cotangent.reshape(MB * N_DP, TOK_DEV, D)
    grad_list = [None] * N_SECTION
    key_list = [None] * N_SECTION
    value_list = [None] * N_SECTION
    gain_list = [None] * N_SECTION
    for section_index in range(N_SECTION - 1, -1, -1):
        x_rows = inputs[section_index].reshape(MB * N_DP, TOK_DEV, D)
        saved = forward(x_rows, norm_gain[section_index], key_weight[section_index], value_weight[section_index])
        lower_grad, key_back, value_flat, gain_term = backward(upper_grad, *saved, norm_gain[section_index], key_weight[section_index], value_weight[section_index])
        normed = saved[2]
        start = (jnp.zeros((D, KV), jnp.float32), jnp.zeros((D, KV), jnp.float32), jnp.zeros((D,), jnp.float32))
        totals, unused = lax.scan(add_group, start, (regroup(normed), regroup(key_back), regroup(value_flat), regroup(gain_term)))
        key_list[section_index] = totals[0]
        value_list[section_index] = totals[1]
        gain_list[section_index] = totals[2]
        blocks = lower_grad.reshape(MB, TOKENS, D)
        grad_list[section_index] = blocks[plan[section_index]]
        upper_grad = lower_grad
    return (jnp.stack(grad_list), jnp.stack(key_list), jnp.stack(value_list), jnp.stack(gain_list))
```

```python
import functools
import math

import jax
import jax.numpy as jnp
import numpy as np
from jax import lax
from jax.experimental import pallas as pl
from jax.experimental.pallas import tpu as pltpu
from jax.sharding import PartitionSpec as P

HEAD_DIM = 128
EPS = 1e-05
ROPE_BASE = 500000.0
PIECES = 2
MESH = pl.DeviceIdType.MESH
F32 = jnp.float32
BF16 = jnp.bfloat16


def dot_nn(a, b):
    return lax.dot_general(a, b, (((1,), (0,)), ((), ())), preferred_element_type=F32)


def dot_nt(a, b):
    return lax.dot_general(a, b, (((1,), (1,)), ((), ())), preferred_element_type=F32)


def dot_tn(a, b):
    return lax.dot_general(a, b, (((0,), (0,)), ((), ())), preferred_element_type=F32)


def rope_tables(length):
    half = HEAD_DIM // 2
    freq = (ROPE_BASE ** (-(np.arange(half, dtype=np.float32) * 2.0 / HEAD_DIM))).astype(np.float32)
    angles = np.arange(length, dtype=np.float32)[:, None] * freq[None, :]
    cos, sin = np.cos(angles), np.sin(angles)
    return (
        np.concatenate([cos, cos], -1).astype(np.float32),
        np.concatenate([-sin, sin], -1).astype(np.float32),
    )


def kernel(S, N, x_ref, cot_ref, gain_ref, wk_ref, wv_ref, cos_ref, sin_ref,
           low_out, gk_out, gv_out, gg_out,
           wall, ns, nall, gall, inv_s, acc, key_s, val_s, qst, prob, ubuf, lowb, gnb,
           kball, gsh, gsall,
           loc, ws, wr, rls, rlr, gsem, nsem, ssem, us, ur, uloc, kbs, kbr, krs, krr):
    B, KH, L = ubuf.shape[0], ubuf.shape[1], ubuf.shape[2]
    CW = ubuf.shape[3]
    w = wall.shape[1]
    KV = KH * HEAD_DIM
    G = CW // HEAD_DIM
    D = x_ref.shape[1]
    C = N // 2
    scale = 1.0 / math.sqrt(HEAD_DIM)
    sec = lax.axis_index("section")
    me = lax.axis_index("dp")
    c = me // 2
    core = me % 2
    partner = c * 2 + (1 - core)
    hp = w // PIECES

    def remote(src, dst, send, recv, peer):
        return pltpu.make_async_remote_copy(
            src_ref=src, dst_ref=dst, send_sem=send, recv_sem=recv,
            device_id=(sec, peer), device_id_type=MESH)

    def wait_all(ref, sem):
        pltpu.make_async_copy(ref, ref, sem).wait()

    ck = pltpu.make_async_copy(wk_ref, wall.at[me, :, pl.ds(0, KV)], loc.at[0])
    cv = pltpu.make_async_copy(wv_ref, wall.at[me, :, pl.ds(KV, KV)], loc.at[1])
    ck.start()
    cv.start()

    barrier = pltpu.get_barrier_semaphore()
    for i in range(1, N):
        pl.semaphore_signal(barrier, inc=1, device_id=(sec, (me + i) % N), device_id_type=MESH)

    @pl.when(sec > 0)
    def _():
        pl.semaphore_signal(barrier, inc=1, device_id=(sec - 1, me), device_id_type=MESH)

    @pl.when(sec < S - 1)
    def _():
        pl.semaphore_signal(barrier, inc=1, device_id=(sec + 1, me), device_id_type=MESH)
    below = jnp.where(sec > 0, 1, 0)
    above = jnp.where(sec < S - 1, 1, 0)
    pl.semaphore_wait(barrier, N - 1 + below + above)

    gcopies = []
    for i in range(1, N):
        cp = remote(gain_ref, gall.at[me], gsem.at[0], gsem.at[1], (me + i) % N)
        cp.start()
        gcopies.append(cp)
    gall[me] = gain_ref[...]
    ck.wait()
    cv.wait()

    def piece(shard, p):
        return wall.at[shard, pl.ds(p * hp, hp)]

    def wcopy(way, t, p):
        chip = c - t if way == 0 else c + t
        peer = (c + 1 if way == 0 else c - 1) * 2 + core
        ref = piece(chip * 2 + core, p)
        return remote(ref, ref, ws.at[way, t, p], wr.at[way, t, p], peer)

    def wrecv(way, t, p):
        chip = c - 1 - t if way == 0 else c + 1 + t
        ref = piece(chip * 2 + core, p)
        return remote(ref, ref, ws.at[way, t, p], wr.at[way, t, p], partner)

    def relay(slot, chip, p, mine):
        ref = piece(chip * 2 + (core if mine else 1 - core), p)
        return remote(ref, ref, rls.at[slot, p], rlr.at[slot, p], partner)

    def can_send(way, t):
        return ((c - t >= 0) & (c + 1 < C)) if way == 0 else ((c + t < C) & (c >= 1))

    def can_recv(way, t):
        return (c - 1 - t >= 0) if way == 0 else (c + 1 + t < C)

    for p in range(PIECES):
        for way in range(2):
            @pl.when(can_send(way, 0))
            def _(way=way, p=p):
                wcopy(way, 0, p).start()
        relay(0, c, p, True).start()

    def cot_copy(k, j):
        return pltpu.make_async_copy(
            cot_ref.at[k, :, pl.ds(j * CW, CW)], ubuf.at[k, j], uloc.at[k, j])

    @pl.when(sec == S - 1)
    def _():
        for k in range(B):
            for j in range(KH):
                cot_copy(k, j).start()

    total = jnp.zeros((B * L, 1), F32)
    for d in range(N):
        xd = x_ref[:, d * w:(d + 1) * w].astype(F32)
        total = total + jnp.sum(xd * xd, axis=-1, keepdims=True)
    inv = lax.rsqrt(total * (1.0 / D) + EPS)
    inv_s[...] = jnp.broadcast_to(inv, inv_s.shape)
    wait_all(gall.at[pl.ds(0, N - 1)], gsem.at[1])
    for d in range(N):
        xd = x_ref[:, d * w:(d + 1) * w].astype(F32)
        ns[d] = (xd * inv * gall[d][0:1, :]).astype(BF16)
        gsh[d] = jnp.zeros(gsh.shape[1:], F32)
    nall[me] = ns[me]
    cos = cos_ref[...]
    sin = sin_ref[...]

    def queries(k, carry):
        rows = pl.ds(pl.multiple_of(k * L, L), L)
        for j in range(KH):
            for g in range(G):
                col = (j * G + g) * HEAD_DIM
                v = ns[col // w, rows, col % w:col % w + HEAD_DIM].astype(F32)
                q = v * cos + pltpu.roll(v, HEAD_DIM // 2, 1) * sin
                qst[k, j, g * L:(g + 1) * L, :] = q.astype(BF16)
        return carry
    lax.fori_loop(0, B, queries, 0)

    def forward_step(t):
        for p in range(PIECES):
            for way in range(2):
                @pl.when(can_recv(way, t))
                def _(way=way, p=p):
                    wrecv(way, t, p).wait_recv()
                    if t + 1 < C - 1:
                        @pl.when(can_send(way, t + 1))
                        def _():
                            wcopy(way, t + 1, p).start()
                    chip = c - 1 - t if way == 0 else c + 1 + t
                    relay(1 + way * (C - 1) + t, chip, p, True).start()

    def use_step(t):
        for way in range(2):
            @pl.when(can_recv(way, t))
            def _(way=way):
                chip = c - 1 - t if way == 0 else c + 1 + t
                for p in range(PIECES):
                    relay(1 + way * (C - 1) + t, chip, p, False).wait_recv()
                acc[...] += dot_nn(ns[chip * 2], wall[chip * 2]) + dot_nn(
                    ns[chip * 2 + 1], wall[chip * 2 + 1])

    forward_step(0)
    for p in range(PIECES):
        relay(0, c, p, False).wait_recv()
    acc[...] = dot_nn(ns[c * 2], wall[c * 2]) + dot_nn(ns[c * 2 + 1], wall[c * 2 + 1])
    for t in range(C - 1):
        if t + 1 < C - 1:
            forward_step(t + 1)
        use_step(t)

    for i in range(1, N):
        peer = (me + i) % N
        remote(ns.at[peer], nall.at[me], nsem.at[0], nsem.at[1], peer).start()

    row_pos = lax.broadcasted_iota(jnp.int32, (L, L), 0)
    col_pos = lax.broadcasted_iota(jnp.int32, (L, L), 1)
    causal = (row_pos >= col_pos)[None]

    def attend(k, carry):
        rows = pl.ds(pl.multiple_of(k * L, L), L)
        for j in range(KH):
            kp = acc[rows, j * HEAD_DIM:(j + 1) * HEAD_DIM]
            key = (kp * cos + pltpu.roll(kp, HEAD_DIM // 2, 1) * sin).astype(BF16)
            key_s[k, j] = key
            val_s[k, j] = acc[rows, KV + j * HEAD_DIM:KV + (j + 1) * HEAD_DIM].astype(BF16)
            sc = dot_nt(qst[k, j], key) * scale
            raised = jnp.where(causal, jnp.exp(sc.reshape(G, L, L)), 0.0)
            pr = raised / jnp.sum(raised, axis=-1, keepdims=True)
            prob[k, j] = pr.reshape(G * L, L)
        return carry
    lax.fori_loop(0, B, attend, 0)

    def usend(k, j):
        return pltpu.make_async_remote_copy(
            src_ref=lowb.at[k, j], dst_ref=ubuf.at[k, j], send_sem=us.at[k, j],
            recv_sem=ur.at[k, j], device_id=(lax.max(sec - 1, 0), me), device_id_type=MESH)

    def kbcopy(k, j, i):
        peer = ((c + i) % C) * 2 + core
        ref = kball.at[me, k, j]
        return remote(ref, ref, kbs.at[k, i], kbr.at[k, i], peer)

    def kbpartner(k, j):
        ref = kball.at[me, k, j]
        return remote(ref, ref, kbs.at[k, 0], kbr.at[k, 0], partner)

    def kbrelay(k, i, mine):
        chip = (c - i + C) % C
        ref = kball.at[chip * 2 + (core if mine else 1 - core), k]
        return remote(ref, ref, krs.at[k, i], krr.at[k, i], partner)

    def turn(k, carry):
        rows = pl.ds(pl.multiple_of(k * L, L), L)
        keys, values = [], []
        for j in range(KH):
            @pl.when(sec == S - 1)
            def _(j=j):
                cot_copy(k, j).wait()

            @pl.when(sec < S - 1)
            def _(j=j):
                usend(k, j).wait_recv()
            u = ubuf[k, j]
            us_ = jnp.concatenate(
                [u[:, g * HEAD_DIM:(g + 1) * HEAD_DIM] for g in range(G)], axis=0)
            key, q, pr = key_s[k, j], qst[k, j], prob[k, j]
            gp = dot_nt(us_, val_s[k, j])
            gv = dot_tn(pr.astype(BF16), us_).astype(BF16)
            rd = jnp.sum(pr * gp, axis=-1, keepdims=True)
            gs = (pr * (gp - rd) * scale).astype(BF16)
            gk = dot_tn(gs, q)
            gk = (gk * cos - pltpu.roll(gk, HEAD_DIM // 2, 1) * sin).astype(BF16)
            keys.append(gk)
            values.append(gv)
            kball[me, k, j] = jnp.concatenate([gk, gv], axis=1)
            gq = dot_nn(gs, key)
            for g in range(G):
                v = gq[g * L:(g + 1) * L]
                col = (j * G + g) * HEAD_DIM
                gnb[col // w, :, col % w:col % w + HEAD_DIM] = (
                    v * cos - pltpu.roll(v, HEAD_DIM // 2, 1) * sin)
            kbpartner(k, j).start()
            for i in range(1, C):
                kbcopy(k, j, i).start()
        kbv = jnp.concatenate(keys + values, axis=1)
        part_inv = inv_s[rows, 0:1]
        proj = jnp.zeros((L, 1), F32)
        for d in range(N):
            gn = gnb[d] + dot_nt(kbv, wall[d])
            gnb[d] = gn
            gt = gn * x_ref[rows, d * w:(d + 1) * w].astype(F32) * part_inv
            proj = proj + jnp.sum(gt * gall[d][0:1, :], axis=-1, keepdims=True)
            gsh[d] += jnp.sum(gt.reshape(L // 8, 8, w), axis=0)
        proj = proj * (1.0 / D) * part_inv * part_inv
        for j in range(KH):
            for e in range(N // KH):
                d = j * (N // KH) + e
                u = ubuf[k, j, :, e * w:(e + 1) * w].astype(F32)
                xd = x_ref[rows, d * w:(d + 1) * w].astype(F32)
                low = (u + part_inv * gall[d][0:1, :] * gnb[d] - xd * proj).astype(BF16)
                lowb[k, j, :, e * w:(e + 1) * w] = low
                low_out[rows, d * w:(d + 1) * w] = low

            @pl.when(sec > 0)
            def _(j=j):
                usend(k, j).start()
        return carry
    lax.fori_loop(0, B, turn, 0)

    gsall[me] = gsh[me]
    for i in range(1, N):
        peer = (me + i) % N
        remote(gsh.at[peer], gsall.at[me], ssem.at[0], ssem.at[1], peer).start()
    for k in range(B):
        for i in range(1, C):
            chip = (c - i + C) % C
            wait_all(kball.at[chip * 2 + core, k], kbr.at[k, i])
            kbrelay(k, i, True).start()
    wait_all(nall.at[pl.ds(0, N - 1)], nsem.at[1])
    for k in range(B):
        wait_all(kball.at[partner, k], kbr.at[k, 0])
        for i in range(1, C):
            kbrelay(k, i, False).wait_recv()
    rows_all = nall[...].reshape(N * B * L, w)
    for j in range(KH):
        back = jnp.concatenate(
            [kball[g, k, j] for g in range(N) for k in range(B)], axis=0)
        dw = dot_tn(rows_all, back)
        gk_out[:, j * HEAD_DIM:(j + 1) * HEAD_DIM] = dw[:, :HEAD_DIM]
        gv_out[:, j * HEAD_DIM:(j + 1) * HEAD_DIM] = dw[:, HEAD_DIM:]
    wait_all(gsall.at[pl.ds(0, N - 1)], ssem.at[1])
    gg = gsall[0]
    for d in range(1, N):
        gg = gg + gsall[d]
    gg_out[...] = jnp.broadcast_to(jnp.sum(gg, axis=0, keepdims=True), gg_out.shape)

    wait_all(gall.at[pl.ds(0, N - 1)], gsem.at[0])
    wait_all(nall.at[pl.ds(0, N - 1)], nsem.at[0])
    wait_all(gsall.at[pl.ds(0, N - 1)], ssem.at[0])
    for p in range(PIECES):
        relay(0, c, p, True).wait_send()
        for way in range(2):
            for t in range(C - 1):
                @pl.when(can_send(way, t))
                def _(way=way, t=t, p=p):
                    wcopy(way, t, p).wait_send()

                @pl.when(can_recv(way, t))
                def _(way=way, t=t, p=p):
                    chip = c - 1 - t if way == 0 else c + 1 + t
                    relay(1 + way * (C - 1) + t, chip, p, True).wait_send()
    for k in range(B):
        for i in range(C):
            wait_all(kball.at[me, k], kbs.at[k, i])
            if i:
                kbrelay(k, i, True).wait_send()

    @pl.when(sec > 0)
    def _():
        for k in range(B):
            for j in range(KH):
                usend(k, j).wait_send()


def body(S, N, inputs, cotangent, norm_gain, key_weight, value_weight, plan):
    B, L, D = inputs.shape[1:]
    w, KV = key_weight.shape[1:]
    KH = KV // HEAD_DIM
    CW = D // KH
    G = CW // HEAD_DIM
    C = N // 2
    cos, sin = rope_tables(L)
    gain8 = jnp.broadcast_to(norm_gain.astype(F32), (8, w))
    vmem = pl.BlockSpec(memory_space=pltpu.VMEM)
    hbm = pl.BlockSpec(memory_space=pl.ANY)
    dma = pltpu.SemaphoreType.DMA
    low, gk, gv, gg = pl.pallas_call(
        functools.partial(kernel, S, N),
        out_shape=(
            jax.ShapeDtypeStruct((B * L, D), BF16),
            jax.ShapeDtypeStruct((w, KV), F32),
            jax.ShapeDtypeStruct((w, KV), F32),
            jax.ShapeDtypeStruct((8, w), F32),
        ),
        in_specs=[vmem, hbm, vmem, hbm, hbm, vmem, vmem],
        out_specs=(vmem,) * 4,
        scratch_shapes=[
            pltpu.VMEM((N, w, 2 * KV), BF16),
            pltpu.VMEM((N, B * L, w), BF16),
            pltpu.VMEM((N, B * L, w), BF16),
            pltpu.VMEM((N, 8, w), F32),
            pltpu.VMEM((B * L, 128), F32),
            pltpu.VMEM((B * L, 2 * KV), F32),
            pltpu.VMEM((B, KH, L, HEAD_DIM), BF16),
            pltpu.VMEM((B, KH, L, HEAD_DIM), BF16),
            pltpu.VMEM((B, KH, G * L, HEAD_DIM), BF16),
            pltpu.VMEM((B, KH, G * L, L), F32),
            pltpu.VMEM((B, KH, L, CW), BF16),
            pltpu.VMEM((B, KH, L, CW), BF16),
            pltpu.VMEM((N, L, w), F32),
            pltpu.VMEM((N, B, KH, L, 2 * HEAD_DIM), BF16),
            pltpu.VMEM((N, 8, w), F32),
            pltpu.VMEM((N, 8, w), F32),
            dma((2,)),
            dma((2, C - 1, PIECES)),
            dma((2, C - 1, PIECES)),
            dma((2 * C - 1, PIECES)),
            dma((2 * C - 1, PIECES)),
            dma((2,)),
            dma((2,)),
            dma((2,)),
            dma((B, KH)),
            dma((B, KH)),
            dma((B, KH)),
            dma((B, C)),
            dma((B, C)),
            dma((B, C)),
            dma((B, C)),
        ],
        compiler_params=pltpu.CompilerParams(
            collective_id=0, has_side_effects=True, vmem_limit_bytes=56 * 1024 * 1024),
    )(inputs[0].reshape(B * L, D), cotangent, gain8, key_weight[0], value_weight[0],
      jnp.asarray(cos), jnp.asarray(sin))
    low = low.reshape(B, L, D)
    selector = plan[0][:, None] == jnp.arange(B, dtype=jnp.int32)[None, :]
    ordered = jnp.sum(
        jnp.where(selector[:, :, None, None], low[None], jnp.zeros((), BF16)), axis=1)
    return ordered[None], gk[None], gv[None], gg[0:1]


def solution(mesh):
    in_specs = (
        P("section", None, "dp", None),
        P(None, "dp", None),
        P("section", "dp"),
        P("section", "dp", None),
        P("section", "dp", None),
        P("section", None),
    )
    out_specs = (
        P("section", None, "dp", None),
        P("section", "dp", None),
        P("section", "dp", None),
        P("section", "dp"),
    )
    run = functools.partial(body, mesh.shape["section"], mesh.shape["dp"])
    return jax.shard_map(run, mesh=mesh, in_specs=in_specs, out_specs=out_specs, check_vma=False)
```

```python
import functools
import math

import jax
import jax.numpy as jnp
import numpy as np
from jax import lax
from jax.experimental import pallas as pl
from jax.experimental.pallas import tpu as pltpu
from jax.sharding import PartitionSpec as P

HEAD_DIM = 128
EPS = 1e-05
ROPE_BASE = 500000.0
PIECES = 4
HELPED = 1
MESH = pl.DeviceIdType.MESH
F32 = jnp.float32
BF16 = jnp.bfloat16


def dot_nn(a, b):
    return lax.dot_general(a, b, (((1,), (0,)), ((), ())), preferred_element_type=F32)


def dot_nt(a, b):
    return lax.dot_general(a, b, (((1,), (1,)), ((), ())), preferred_element_type=F32)


def dot_tn(a, b):
    return lax.dot_general(a, b, (((0,), (0,)), ((), ())), preferred_element_type=F32)


def rope_tables(length):
    half = HEAD_DIM // 2
    freq = (ROPE_BASE ** (-(np.arange(half, dtype=np.float32) * 2.0 / HEAD_DIM))).astype(np.float32)
    angles = np.arange(length, dtype=np.float32)[:, None] * freq[None, :]
    cos, sin = np.cos(angles), np.sin(angles)
    return (
        np.concatenate([cos, cos], -1).astype(np.float32),
        np.concatenate([-sin, sin], -1).astype(np.float32),
    )


def kernel(S, N, x_ref, cot_ref, gain_ref, wk_ref, wv_ref, cos_ref, sin_ref,
           low_out, gk_out, gv_out, gg_out,
           wall, ns, nall, gall, inv_s, acc, key_s, val_s, qst, prob, ubuf, lowb, gnb,
           kball, gsh, gsall, stage,
           loc, ws, wr, hs, hr, ps, pr_sem, token, rls, rlr, gsem, nsem, ssem, us, ur, uloc, kbs, kbr, krs, krr):
    B, KH, L = ubuf.shape[0], ubuf.shape[1], ubuf.shape[2]
    CW = ubuf.shape[3]
    w = wall.shape[1]
    KV = KH * HEAD_DIM
    G = CW // HEAD_DIM
    D = x_ref.shape[1]
    C = N // 2
    scale = 1.0 / math.sqrt(HEAD_DIM)
    sec = lax.axis_index("section")
    me = lax.axis_index("dp")
    c = me // 2
    core = me % 2
    partner = c * 2 + (1 - core)
    hp = w // PIECES
    OWN = PIECES - HELPED if S % 2 == 0 else PIECES
    upper = sec >= S // 2
    pair = jnp.where(upper, sec - S // 2, sec + S // 2) if S % 2 == 0 else sec

    def remote(src, dst, send, recv, peer):
        return pltpu.make_async_remote_copy(
            src_ref=src, dst_ref=dst, send_sem=send, recv_sem=recv,
            device_id=(sec, peer), device_id_type=MESH)

    def wait_all(ref, sem):
        pltpu.make_async_copy(ref, ref, sem).wait()

    ck = pltpu.make_async_copy(wk_ref, wall.at[me, :, pl.ds(0, KV)], loc.at[0])
    cv = pltpu.make_async_copy(wv_ref, wall.at[me, :, pl.ds(KV, KV)], loc.at[1])
    ck.start()
    cv.start()

    barrier = pltpu.get_barrier_semaphore()
    for i in range(1, N):
        pl.semaphore_signal(barrier, inc=1, device_id=(sec, (me + i) % N), device_id_type=MESH)

    @pl.when(sec > 0)
    def _():
        pl.semaphore_signal(barrier, inc=1, device_id=(sec - 1, me), device_id_type=MESH)

    @pl.when(sec < S - 1)
    def _():
        pl.semaphore_signal(barrier, inc=1, device_id=(sec + 1, me), device_id_type=MESH)
    helps = S % 2 == 0 and S > 2
    if helps:
        pl.semaphore_signal(barrier, inc=1, device_id=(pair, me), device_id_type=MESH)
    below = jnp.where(sec > 0, 1, 0)
    above = jnp.where(sec < S - 1, 1, 0)
    pl.semaphore_wait(barrier, N - 1 + below + above + (1 if helps else 0))

    gcopies = []
    for i in range(1, N):
        cp = remote(gain_ref, gall.at[me], gsem.at[0], gsem.at[1], (me + i) % N)
        cp.start()
        gcopies.append(cp)
    gall[me] = gain_ref[...]
    ck.wait()
    cv.wait()

    def piece(shard, p):
        return wall.at[shard, pl.ds(p * hp, hp)]

    def wcopy(way, t, p):
        chip = c - t if way == 0 else c + t
        peer = (c + 1 if way == 0 else c - 1) * 2 + core
        ref = piece(chip * 2 + core, p)
        return remote(ref, ref, ws.at[way, t, p], wr.at[way, t, p], peer)

    def wrecv(way, t, p):
        chip = c - 1 - t if way == 0 else c + 1 + t
        ref = piece(chip * 2 + core, p)
        return remote(ref, ref, ws.at[way, t, p], wr.at[way, t, p], partner)

    def relay(slot, chip, p, mine):
        ref = piece(chip * 2 + (core if mine else 1 - core), p)
        return remote(ref, ref, rls.at[slot], rlr.at[slot], partner)

    def relayed(slot, chip, mine, sem):
        wait_all(wall.at[chip * 2 + (core if mine else 1 - core)], sem.at[slot])

    def to_pair(p):
        return pltpu.make_async_remote_copy(
            src_ref=piece(me, p), dst_ref=stage.at[c, p - OWN], send_sem=ps.at[0, p - OWN],
            recv_sem=pr_sem.at[0, p - OWN], device_id=(pair, me), device_id_type=MESH)

    def hcopy(way, t, p, receive=False):
        if receive:
            chip, peer = (c - 1 - t if way == 0 else c + 1 + t), partner
        else:
            chip = c - t if way == 0 else c + t
            peer = (c + 1 if way == 0 else c - 1) * 2 + core
        ref = stage.at[chip, p - OWN]
        return remote(ref, ref, hs.at[way, t, p - OWN], hr.at[way, t, p - OWN], peer)

    def hand(way, t, p):
        chip = c - 1 - t if way == 0 else c + 1 + t
        slot = 1 + way * (C - 1) + t
        return pltpu.make_async_remote_copy(
            src_ref=stage.at[chip, p - OWN], dst_ref=piece(chip * 2 + core, p),
            send_sem=ps.at[slot, p - OWN], recv_sem=pr_sem.at[slot, p - OWN],
            device_id=(pair, me), device_id_type=MESH)

    def can_send(way, t):
        return ((c - t >= 0) & (c + 1 < C)) if way == 0 else ((c + t < C) & (c >= 1))

    def can_recv(way, t):
        return (c - 1 - t >= 0) if way == 0 else (c + 1 + t < C)

    for p in range(OWN, PIECES):
        @pl.when(upper)
        def _(p=p):
            to_pair(p).start()
    for p in range(OWN):
        for way in range(2):
            @pl.when(can_send(way, 0) & upper)
            def _(way=way, p=p):
                wcopy(way, 0, p).start()
    for p in range(PIECES):
        relay(0, c, p, True).start()

    def cot_copy(k, j):
        return pltpu.make_async_copy(
            cot_ref.at[k, :, pl.ds(j * CW, CW)], ubuf.at[k, j], uloc.at[k, j])

    @pl.when(sec == S - 1)
    def _():
        for k in range(B):
            for j in range(KH):
                cot_copy(k, j).start()

    total = jnp.zeros((B * L, 1), F32)
    for d in range(N):
        xd = x_ref[:, d * w:(d + 1) * w].astype(F32)
        total = total + jnp.sum(xd * xd, axis=-1, keepdims=True)
    inv = lax.rsqrt(total * (1.0 / D) + EPS)
    inv_s[...] = jnp.broadcast_to(inv, inv_s.shape)
    wait_all(gall.at[pl.ds(0, N - 1)], gsem.at[1])
    for d in range(N):
        xd = x_ref[:, d * w:(d + 1) * w].astype(F32)
        ns[d] = (xd * inv * gall[d][0:1, :]).astype(BF16)
        gsh[d] = jnp.zeros(gsh.shape[1:], F32)
    nall[me] = ns[me]
    cos = cos_ref[...]
    sin = sin_ref[...]

    def queries(k, carry):
        rows = pl.ds(pl.multiple_of(k * L, L), L)
        for j in range(KH):
            for g in range(G):
                col = (j * G + g) * HEAD_DIM
                v = ns[col // w, rows, col % w:col % w + HEAD_DIM].astype(F32)
                q = v * cos + pltpu.roll(v, HEAD_DIM // 2, 1) * sin
                qst[k, j, g * L:(g + 1) * L, :] = q.astype(BF16)
        return carry
    lax.fori_loop(0, B, queries, 0)

    def forward_step(t):
        for p in range(PIECES):
            for way in range(2):
                chip = c - 1 - t if way == 0 else c + 1 + t

                @pl.when(can_recv(way, t))
                def _(way=way, p=p, chip=chip):
                    def by_line():
                        wrecv(way, t, p).wait_recv()
                        if t + 1 < C - 1:
                            @pl.when(can_send(way, t + 1))
                            def _():
                                wcopy(way, t + 1, p).start()
                    if p < OWN:
                        by_line()
                    else:
                        @pl.when(upper)
                        def _():
                            hand(way, t, p).wait_recv()

                        @pl.when(jnp.logical_not(upper))
                        def _():
                            by_line()
                    relay(1 + way * (C - 1) + t, chip, p, True).start()

    def use_step(t):
        for way in range(2):
            @pl.when(can_recv(way, t))
            def _(way=way):
                chip = c - 1 - t if way == 0 else c + 1 + t
                relayed(1 + way * (C - 1) + t, chip, False, rlr)
                acc[...] += dot_nn(ns[chip * 2], wall[chip * 2]) + dot_nn(
                    ns[chip * 2 + 1], wall[chip * 2 + 1])

    @pl.when(jnp.logical_not(upper))
    def _():
        for t in range(C - 1):
            for p in range(OWN, PIECES):
                if t == 0:
                    to_pair(p).wait_recv()
                for way in range(2):
                    if t == 0:
                        @pl.when(can_send(way, 0))
                        def _(way=way, p=p):
                            hcopy(way, 0, p).start()
            for p in range(OWN, PIECES):
                for way in range(2):
                    if t + 1 == C - 1:
                        for q in range(PIECES) if p == OWN else ():
                            @pl.when(can_send(way, 0))
                            def _(way=way, q=q):
                                wcopy(way, 0, q).start()
            for p in range(OWN, PIECES):
                for way in range(2):
                    @pl.when(can_recv(way, t))
                    def _(way=way, p=p, t=t):
                        hcopy(way, t, p, True).wait_recv()
                        if t + 1 < C - 1:
                            @pl.when(can_send(way, t + 1))
                            def _():
                                hcopy(way, t + 1, p).start()
                        hand(way, t, p).start()

    forward_step(0)
    relayed(0, c, False, rlr)
    acc[...] = dot_nn(ns[c * 2], wall[c * 2]) + dot_nn(ns[c * 2 + 1], wall[c * 2 + 1])
    for t in range(C - 1):
        if t + 1 < C - 1:
            forward_step(t + 1)
        use_step(t)

    for i in range(1, N):
        peer = (me + i) % N
        remote(ns.at[peer], nall.at[me], nsem.at[0], nsem.at[1], peer).start()

    row_pos = lax.broadcasted_iota(jnp.int32, (L, L), 0)
    col_pos = lax.broadcasted_iota(jnp.int32, (L, L), 1)
    causal = (row_pos >= col_pos)[None]

    def attend(k, carry):
        rows = pl.ds(pl.multiple_of(k * L, L), L)
        for j in range(KH):
            kp = acc[rows, j * HEAD_DIM:(j + 1) * HEAD_DIM]
            key = (kp * cos + pltpu.roll(kp, HEAD_DIM // 2, 1) * sin).astype(BF16)
            key_s[k, j] = key
            val_s[k, j] = acc[rows, KV + j * HEAD_DIM:KV + (j + 1) * HEAD_DIM].astype(BF16)
            sc = dot_nt(qst[k, j], key) * scale
            raised = jnp.where(causal, jnp.exp(sc.reshape(G, L, L)), 0.0)
            pr = raised / jnp.sum(raised, axis=-1, keepdims=True)
            prob[k, j] = pr.reshape(G * L, L)
        return carry
    lax.fori_loop(0, B, attend, 0)

    def usend(k, j):
        return pltpu.make_async_remote_copy(
            src_ref=lowb.at[k, j], dst_ref=ubuf.at[k, j], send_sem=us.at[k, j],
            recv_sem=ur.at[k, j], device_id=(lax.max(sec - 1, 0), me), device_id_type=MESH)

    def kbcopy(k, j, i):
        peer = ((c + i) % C) * 2 + core
        ref = kball.at[me, k, j]
        return remote(ref, ref, kbs.at[k, i], kbr.at[k, i], peer)

    def kbpartner(k, j):
        ref = kball.at[me, k, j]
        return remote(ref, ref, kbs.at[k, 0], kbr.at[k, 0], partner)

    def kbrelay(k, i, mine):
        chip = (c - i + C) % C
        ref = kball.at[chip * 2 + (core if mine else 1 - core), k]
        return remote(ref, ref, krs.at[k, i], krr.at[k, i], partner)

    def sent(k):
        @pl.when(sec > 0)
        def _():
            for j in range(KH):
                usend(k, j).wait_send()

    def turn(k, carry):
        rows = pl.ds(pl.multiple_of(k * L, L), L)
        keys, values = [], []
        for j in range(KH):
            @pl.when(sec == S - 1)
            def _(j=j):
                cot_copy(k, j).wait()

            @pl.when(sec < S - 1)
            def _(j=j):
                usend(k, j).wait_recv()
            u = ubuf[k, j]
            us_ = jnp.concatenate(
                [u[:, g * HEAD_DIM:(g + 1) * HEAD_DIM] for g in range(G)], axis=0)
            key, q, pr = key_s[k, j], qst[k, j], prob[k, j]
            gp = dot_nt(us_, val_s[k, j])
            gv = dot_tn(pr.astype(BF16), us_).astype(BF16)
            rd = jnp.sum(pr * gp, axis=-1, keepdims=True)
            gs = (pr * (gp - rd) * scale).astype(BF16)
            gk = dot_tn(gs, q)
            gk = (gk * cos - pltpu.roll(gk, HEAD_DIM // 2, 1) * sin).astype(BF16)
            keys.append(gk)
            values.append(gv)
            kball[me, k, j] = jnp.concatenate([gk, gv], axis=1)
            gq = dot_nn(gs, key)
            for g in range(G):
                v = gq[g * L:(g + 1) * L]
                col = (j * G + g) * HEAD_DIM
                gnb[col // w, :, col % w:col % w + HEAD_DIM] = (
                    v * cos - pltpu.roll(v, HEAD_DIM // 2, 1) * sin)
            kbpartner(k, j).start()
            for i in range(1, C):
                kbcopy(k, j, i).start()
        @pl.when((sec == S - 1) & (k > 0))
        def _():
            sent(k - 1)
            pl.semaphore_signal(token, inc=1, device_id=(sec, partner), device_id_type=MESH)
        kbv = jnp.concatenate(keys + values, axis=1)
        part_inv = inv_s[rows, 0:1]
        proj = jnp.zeros((L, 1), F32)
        for d in range(N):
            gn = gnb[d] + dot_nt(kbv, wall[d])
            gnb[d] = gn
            gt = gn * x_ref[rows, d * w:(d + 1) * w].astype(F32) * part_inv
            proj = proj + jnp.sum(gt * gall[d][0:1, :], axis=-1, keepdims=True)
            gsh[d] += jnp.sum(gt.reshape(L // 8, 8, w), axis=0)
        proj = proj * (1.0 / D) * part_inv * part_inv
        @pl.when((sec == S - 1) & ((k > 0) | (core > 0)))
        def _():
            pl.semaphore_wait(token, 1)
        for j in range(KH):
            for e in range(N // KH):
                d = j * (N // KH) + e
                u = ubuf[k, j, :, e * w:(e + 1) * w].astype(F32)
                xd = x_ref[rows, d * w:(d + 1) * w].astype(F32)
                low = (u + part_inv * gall[d][0:1, :] * gnb[d] - xd * proj).astype(BF16)
                lowb[k, j, :, e * w:(e + 1) * w] = low
                low_out[rows, d * w:(d + 1) * w] = low

            @pl.when(sec > 0)
            def _(j=j):
                usend(k, j).start()
        return carry
    lax.fori_loop(0, B, turn, 0)

    @pl.when((sec == S - 1) & (core == 0))
    def _():
        sent(B - 1)
        pl.semaphore_signal(token, inc=1, device_id=(sec, partner), device_id_type=MESH)

    gsall[me] = gsh[me]
    for i in range(1, N):
        peer = (me + i) % N
        remote(gsh.at[peer], gsall.at[me], ssem.at[0], ssem.at[1], peer).start()
    for k in range(B):
        for i in range(1, C):
            chip = (c - i + C) % C
            wait_all(kball.at[chip * 2 + core, k], kbr.at[k, i])
            kbrelay(k, i, True).start()
    wait_all(nall.at[pl.ds(0, N - 1)], nsem.at[1])
    for k in range(B):
        wait_all(kball.at[partner, k], kbr.at[k, 0])
        for i in range(1, C):
            kbrelay(k, i, False).wait_recv()
    rows_all = nall[...].reshape(N * B * L, w)
    for j in range(KH):
        back = jnp.concatenate(
            [kball[g, k, j] for g in range(N) for k in range(B)], axis=0)
        dw = dot_tn(rows_all, back)
        gk_out[:, j * HEAD_DIM:(j + 1) * HEAD_DIM] = dw[:, :HEAD_DIM]
        gv_out[:, j * HEAD_DIM:(j + 1) * HEAD_DIM] = dw[:, HEAD_DIM:]
    wait_all(gsall.at[pl.ds(0, N - 1)], ssem.at[1])
    gg = gsall[0]
    for d in range(1, N):
        gg = gg + gsall[d]
    gg_out[...] = jnp.broadcast_to(jnp.sum(gg, axis=0, keepdims=True), gg_out.shape)

    wait_all(gall.at[pl.ds(0, N - 1)], gsem.at[0])
    wait_all(nall.at[pl.ds(0, N - 1)], nsem.at[0])
    wait_all(gsall.at[pl.ds(0, N - 1)], ssem.at[0])
    relayed(0, c, True, rls)
    for way in range(2):
        for t in range(C - 1):
            for p in range(PIECES):
                @pl.when(can_send(way, t) if p < OWN else can_send(way, t) & jnp.logical_not(upper))
                def _(way=way, t=t, p=p):
                    wcopy(way, t, p).wait_send()

            @pl.when(can_recv(way, t))
            def _(way=way, t=t):
                chip = c - 1 - t if way == 0 else c + 1 + t
                relayed(1 + way * (C - 1) + t, chip, True, rls)
            for p in range(OWN, PIECES):
                @pl.when(can_send(way, t) & jnp.logical_not(upper))
                def _(way=way, t=t, p=p):
                    hcopy(way, t, p).wait_send()

                @pl.when(can_recv(way, t) & jnp.logical_not(upper))
                def _(way=way, t=t, p=p):
                    hand(way, t, p).wait_send()
    for p in range(OWN, PIECES):
        @pl.when(upper)
        def _(p=p):
            to_pair(p).wait_send()
    for k in range(B):
        for i in range(C):
            wait_all(kball.at[me, k], kbs.at[k, i])
            if i:
                kbrelay(k, i, True).wait_send()

    @pl.when(sec < S - 1)
    def _():
        for k in range(B):
            sent(k)

    @pl.when((sec == S - 1) & (core == 1))
    def _():
        sent(B - 1)


def body(S, N, inputs, cotangent, norm_gain, key_weight, value_weight, plan):
    B, L, D = inputs.shape[1:]
    w, KV = key_weight.shape[1:]
    KH = KV // HEAD_DIM
    CW = D // KH
    G = CW // HEAD_DIM
    C = N // 2
    cos, sin = rope_tables(L)
    gain8 = jnp.broadcast_to(norm_gain.astype(F32), (8, w))
    vmem = pl.BlockSpec(memory_space=pltpu.VMEM)
    hbm = pl.BlockSpec(memory_space=pl.ANY)
    dma = pltpu.SemaphoreType.DMA
    low, gk, gv, gg = pl.pallas_call(
        functools.partial(kernel, S, N),
        out_shape=(
            jax.ShapeDtypeStruct((B * L, D), BF16),
            jax.ShapeDtypeStruct((w, KV), F32),
            jax.ShapeDtypeStruct((w, KV), F32),
            jax.ShapeDtypeStruct((8, w), F32),
        ),
        in_specs=[vmem, hbm, vmem, hbm, hbm, vmem, vmem],
        out_specs=(vmem,) * 4,
        scratch_shapes=[
            pltpu.VMEM((N, w, 2 * KV), BF16),
            pltpu.VMEM((N, B * L, w), BF16),
            pltpu.VMEM((N, B * L, w), BF16),
            pltpu.VMEM((N, 8, w), F32),
            pltpu.VMEM((B * L, 128), F32),
            pltpu.VMEM((B * L, 2 * KV), F32),
            pltpu.VMEM((B, KH, L, HEAD_DIM), BF16),
            pltpu.VMEM((B, KH, L, HEAD_DIM), BF16),
            pltpu.VMEM((B, KH, G * L, HEAD_DIM), BF16),
            pltpu.VMEM((B, KH, G * L, L), F32),
            pltpu.VMEM((B, KH, L, CW), BF16),
            pltpu.VMEM((B, KH, L, CW), BF16),
            pltpu.VMEM((N, L, w), F32),
            pltpu.VMEM((N, B, KH, L, 2 * HEAD_DIM), BF16),
            pltpu.VMEM((N, 8, w), F32),
            pltpu.VMEM((N, 8, w), F32),
            pltpu.VMEM((C, HELPED, w // PIECES, 2 * KV), BF16),
            dma((2,)),
            dma((2, C - 1, PIECES)),
            dma((2, C - 1, PIECES)),
            dma((2, C - 1, HELPED)),
            dma((2, C - 1, HELPED)),
            dma((2 * C - 1, HELPED)),
            dma((2 * C - 1, HELPED)),
            pltpu.SemaphoreType.REGULAR,
            dma((2 * C - 1,)),
            dma((2 * C - 1,)),
            dma((2,)),
            dma((2,)),
            dma((2,)),
            dma((B, KH)),
            dma((B, KH)),
            dma((B, KH)),
            dma((B, C)),
            dma((B, C)),
            dma((B, C)),
            dma((B, C)),
        ],
        compiler_params=pltpu.CompilerParams(
            collective_id=0, has_side_effects=True, vmem_limit_bytes=56 * 1024 * 1024),
    )(inputs[0].reshape(B * L, D), cotangent, gain8, key_weight[0], value_weight[0],
      jnp.asarray(cos), jnp.asarray(sin))
    low = low.reshape(B, L, D)
    selector = plan[0][:, None] == jnp.arange(B, dtype=jnp.int32)[None, :]
    ordered = jnp.sum(
        jnp.where(selector[:, :, None, None], low[None], jnp.zeros((), BF16)), axis=1)
    return ordered[None], gk[None], gv[None], gg[0:1]


def solution(mesh):
    in_specs = (
        P("section", None, "dp", None),
        P(None, "dp", None),
        P("section", "dp"),
        P("section", "dp", None),
        P("section", "dp", None),
        P("section", None),
    )
    out_specs = (
        P("section", None, "dp", None),
        P("section", "dp", None),
        P("section", "dp", None),
        P("section", "dp"),
    )
    run = functools.partial(body, mesh.shape["section"], mesh.shape["dp"])
    return jax.shard_map(run, mesh=mesh, in_specs=in_specs, out_specs=out_specs, check_vma=False)
```

```python
import functools
import math

import jax
import jax.numpy as jnp
import numpy as np
from jax import lax
from jax.experimental import pallas as pl
from jax.experimental.pallas import tpu as pltpu
from jax.sharding import PartitionSpec as P

HEAD_DIM = 128
EPS = 1e-05
ROPE_BASE = 500000.0
PIECES = 4
HELPED = 1
MESH = pl.DeviceIdType.MESH
F32 = jnp.float32
BF16 = jnp.bfloat16


def dot_nn(a, b):
    return lax.dot_general(a, b, (((1,), (0,)), ((), ())), preferred_element_type=F32)


def dot_nt(a, b):
    return lax.dot_general(a, b, (((1,), (1,)), ((), ())), preferred_element_type=F32)


def dot_tn(a, b):
    return lax.dot_general(a, b, (((0,), (0,)), ((), ())), preferred_element_type=F32)


def rope_tables(length):
    half = HEAD_DIM // 2
    freq = (ROPE_BASE ** (-(np.arange(half, dtype=np.float32) * 2.0 / HEAD_DIM))).astype(np.float32)
    angles = np.arange(length, dtype=np.float32)[:, None] * freq[None, :]
    cos, sin = np.cos(angles), np.sin(angles)
    return (
        np.concatenate([cos, cos], -1).astype(np.float32),
        np.concatenate([-sin, sin], -1).astype(np.float32),
    )


def kernel(S, N, x_ref, cot_ref, gain_ref, wk_ref, wv_ref, cos_ref, sin_ref,
           low_out, gk_out, gv_out, gg_out,
           wall, ns, nall, gall, inv_s, acc, key_s, val_s, qst, prob, ubuf, lowb, gnb,
           kball, gsh, gsall, stage,
           loc, ws, wr, hs, hr, ps, pr_sem, token, rls, rlr, gsem, nsem, ssem, us, ur, uloc, kbs, kbr, krs, krr):
    B, KH, L = ubuf.shape[0], ubuf.shape[1], ubuf.shape[2]
    CW = ubuf.shape[3]
    w = wall.shape[1]
    KV = KH * HEAD_DIM
    G = CW // HEAD_DIM
    D = x_ref.shape[1]
    C = N // 2
    scale = 1.0 / math.sqrt(HEAD_DIM)
    sec = lax.axis_index("section")
    me = lax.axis_index("dp")
    c = me // 2
    core = me % 2
    partner = c * 2 + (1 - core)
    hp = w // PIECES
    OWN = PIECES - HELPED if S % 2 == 0 else PIECES
    upper = sec >= S // 2
    pair = jnp.where(upper, sec - S // 2, sec + S // 2) if S % 2 == 0 else sec

    def remote(src, dst, send, recv, peer):
        return pltpu.make_async_remote_copy(
            src_ref=src, dst_ref=dst, send_sem=send, recv_sem=recv,
            device_id=(sec, peer), device_id_type=MESH)

    def wait_all(ref, sem):
        pltpu.make_async_copy(ref, ref, sem).wait()

    ck = pltpu.make_async_copy(wk_ref, wall.at[me, :, pl.ds(0, KV)], loc.at[0])
    cv = pltpu.make_async_copy(wv_ref, wall.at[me, :, pl.ds(KV, KV)], loc.at[1])
    ck.start()
    cv.start()

    barrier = pltpu.get_barrier_semaphore()
    for i in range(1, N):
        pl.semaphore_signal(barrier, inc=1, device_id=(sec, (me + i) % N), device_id_type=MESH)

    @pl.when(sec > 0)
    def _():
        pl.semaphore_signal(barrier, inc=1, device_id=(sec - 1, me), device_id_type=MESH)

    @pl.when(sec < S - 1)
    def _():
        pl.semaphore_signal(barrier, inc=1, device_id=(sec + 1, me), device_id_type=MESH)
    helps = S % 2 == 0 and S > 2
    if helps:
        pl.semaphore_signal(barrier, inc=1, device_id=(pair, me), device_id_type=MESH)
    below = jnp.where(sec > 0, 1, 0)
    above = jnp.where(sec < S - 1, 1, 0)
    pl.semaphore_wait(barrier, N - 1 + below + above + (1 if helps else 0))

    gcopies = []
    for i in range(1, N):
        cp = remote(gain_ref, gall.at[me], gsem.at[0], gsem.at[1], (me + i) % N)
        cp.start()
        gcopies.append(cp)
    gall[me] = gain_ref[...]
    ck.wait()
    cv.wait()

    def piece(shard, p):
        return wall.at[shard, pl.ds(p * hp, hp)]

    def wcopy(way, t, p):
        chip = c - t if way == 0 else c + t
        peer = (c + 1 if way == 0 else c - 1) * 2 + core
        ref = piece(chip * 2 + core, p)
        return remote(ref, ref, ws.at[way, t, p], wr.at[way, t, p], peer)

    def wrecv(way, t, p):
        chip = c - 1 - t if way == 0 else c + 1 + t
        ref = piece(chip * 2 + core, p)
        return remote(ref, ref, ws.at[way, t, p], wr.at[way, t, p], partner)

    def relay(slot, chip, p, mine):
        ref = piece(chip * 2 + (core if mine else 1 - core), p)
        return remote(ref, ref, rls.at[slot], rlr.at[slot], partner)

    def relayed(slot, chip, mine, sem):
        wait_all(wall.at[chip * 2 + (core if mine else 1 - core)], sem.at[slot])

    def to_pair(p):
        return pltpu.make_async_remote_copy(
            src_ref=piece(me, p), dst_ref=stage.at[c, p - OWN], send_sem=ps.at[0, p - OWN],
            recv_sem=pr_sem.at[0, p - OWN], device_id=(pair, me), device_id_type=MESH)

    def hcopy(way, t, p, receive=False):
        if receive:
            chip, peer = (c - 1 - t if way == 0 else c + 1 + t), partner
        else:
            chip = c - t if way == 0 else c + t
            peer = (c + 1 if way == 0 else c - 1) * 2 + core
        ref = stage.at[chip, p - OWN]
        return remote(ref, ref, hs.at[way, t, p - OWN], hr.at[way, t, p - OWN], peer)

    def hand(way, t, p):
        chip = c - 1 - t if way == 0 else c + 1 + t
        slot = 1 + way * (C - 1) + t
        return pltpu.make_async_remote_copy(
            src_ref=stage.at[chip, p - OWN], dst_ref=piece(chip * 2 + core, p),
            send_sem=ps.at[slot, p - OWN], recv_sem=pr_sem.at[slot, p - OWN],
            device_id=(pair, me), device_id_type=MESH)

    def can_send(way, t):
        return ((c - t >= 0) & (c + 1 < C)) if way == 0 else ((c + t < C) & (c >= 1))

    def can_recv(way, t):
        return (c - 1 - t >= 0) if way == 0 else (c + 1 + t < C)

    for p in range(OWN, PIECES):
        @pl.when(upper)
        def _(p=p):
            to_pair(p).start()
    for p in range(OWN):
        for way in range(2):
            @pl.when(can_send(way, 0) & upper)
            def _(way=way, p=p):
                wcopy(way, 0, p).start()
    for p in range(PIECES):
        relay(0, c, p, True).start()

    def cot_copy(k, j):
        return pltpu.make_async_copy(
            cot_ref.at[k, :, pl.ds(j * CW, CW)], ubuf.at[k, j], uloc.at[k, j])

    @pl.when(sec == S - 1)
    def _():
        for k in range(B):
            for j in range(KH):
                cot_copy(k, j).start()

    total = jnp.zeros((B * L, 1), F32)
    for d in range(N):
        xd = x_ref[:, d * w:(d + 1) * w].astype(F32)
        total = total + jnp.sum(xd * xd, axis=-1, keepdims=True)
    inv = lax.rsqrt(total * (1.0 / D) + EPS)
    inv_s[...] = jnp.broadcast_to(inv, inv_s.shape)
    wait_all(gall.at[pl.ds(0, N - 1)], gsem.at[1])
    for d in range(N):
        xd = x_ref[:, d * w:(d + 1) * w].astype(F32)
        ns[d] = (xd * inv * gall[d][0:1, :]).astype(BF16)
        gsh[d] = jnp.zeros(gsh.shape[1:], F32)
    nall[me] = ns[me]
    cos = cos_ref[...]
    sin = sin_ref[...]

    def queries(k, carry):
        rows = pl.ds(pl.multiple_of(k * L, L), L)
        for j in range(KH):
            for g in range(G):
                col = (j * G + g) * HEAD_DIM
                v = ns[col // w, rows, col % w:col % w + HEAD_DIM].astype(F32)
                q = v * cos + pltpu.roll(v, HEAD_DIM // 2, 1) * sin
                qst[k, j, g * L:(g + 1) * L, :] = q.astype(BF16)
        return carry
    lax.fori_loop(0, B, queries, 0)

    def forward_step(t):
        for p in range(PIECES):
            for way in range(2):
                chip = c - 1 - t if way == 0 else c + 1 + t

                @pl.when(can_recv(way, t))
                def _(way=way, p=p, chip=chip):
                    def by_line():
                        wrecv(way, t, p).wait_recv()
                        if t + 1 < C - 1:
                            @pl.when(can_send(way, t + 1))
                            def _():
                                wcopy(way, t + 1, p).start()
                    if p < OWN:
                        by_line()
                    else:
                        @pl.when(upper)
                        def _():
                            hand(way, t, p).wait_recv()

                        @pl.when(jnp.logical_not(upper))
                        def _():
                            by_line()
                    relay(1 + way * (C - 1) + t, chip, p, True).start()

    def use_step(t):
        for way in range(2):
            @pl.when(can_recv(way, t))
            def _(way=way):
                chip = c - 1 - t if way == 0 else c + 1 + t
                relayed(1 + way * (C - 1) + t, chip, False, rlr)
                acc[...] += dot_nn(ns[chip * 2], wall[chip * 2]) + dot_nn(
                    ns[chip * 2 + 1], wall[chip * 2 + 1])

    @pl.when(jnp.logical_not(upper))
    def _():
        for t in range(C - 1):
            for p in range(OWN, PIECES):
                if t == 0:
                    to_pair(p).wait_recv()
                for way in range(2):
                    if t == 0:
                        @pl.when(can_send(way, 0))
                        def _(way=way, p=p):
                            hcopy(way, 0, p).start()
            for p in range(OWN, PIECES):
                for way in range(2):
                    if p == OWN:
                        for q in range(PIECES):
                            if q != t and not (t + 1 == C - 1 and q > t):
                                continue

                            @pl.when(can_send(way, 0))
                            def _(way=way, q=q):
                                wcopy(way, 0, q).start()
            for p in range(OWN, PIECES):
                for way in range(2):
                    @pl.when(can_recv(way, t))
                    def _(way=way, p=p, t=t):
                        hcopy(way, t, p, True).wait_recv()
                        if t + 1 < C - 1:
                            @pl.when(can_send(way, t + 1))
                            def _():
                                hcopy(way, t + 1, p).start()
                        hand(way, t, p).start()

    forward_step(0)
    relayed(0, c, False, rlr)
    acc[...] = dot_nn(ns[c * 2], wall[c * 2]) + dot_nn(ns[c * 2 + 1], wall[c * 2 + 1])
    for t in range(C - 1):
        if t + 1 < C - 1:
            forward_step(t + 1)
        use_step(t)

    for i in range(1, N):
        peer = (me + i) % N
        remote(ns.at[peer], nall.at[me], nsem.at[0], nsem.at[1], peer).start()

    row_pos = lax.broadcasted_iota(jnp.int32, (L, L), 0)
    col_pos = lax.broadcasted_iota(jnp.int32, (L, L), 1)
    causal = (row_pos >= col_pos)[None]

    def attend(k, carry):
        rows = pl.ds(pl.multiple_of(k * L, L), L)
        for j in range(KH):
            kp = acc[rows, j * HEAD_DIM:(j + 1) * HEAD_DIM]
            key = (kp * cos + pltpu.roll(kp, HEAD_DIM // 2, 1) * sin).astype(BF16)
            key_s[k, j] = key
            val_s[k, j] = acc[rows, KV + j * HEAD_DIM:KV + (j + 1) * HEAD_DIM].astype(BF16)
            sc = dot_nt(qst[k, j], key) * scale
            raised = jnp.where(causal, jnp.exp(sc.reshape(G, L, L)), 0.0)
            pr = raised / jnp.sum(raised, axis=-1, keepdims=True)
            prob[k, j] = pr.reshape(G * L, L)
        return carry
    lax.fori_loop(0, B, attend, 0)

    def usend(k, j):
        return pltpu.make_async_remote_copy(
            src_ref=lowb.at[k, j], dst_ref=ubuf.at[k, j], send_sem=us.at[k, j],
            recv_sem=ur.at[k, j], device_id=(lax.max(sec - 1, 0), me), device_id_type=MESH)

    def kbcopy(k, j, i):
        peer = ((c + i) % C) * 2 + core
        ref = kball.at[me, k, j]
        return remote(ref, ref, kbs.at[k, i], kbr.at[k, i], peer)

    def kbpartner(k, j):
        ref = kball.at[me, k, j]
        return remote(ref, ref, kbs.at[k, 0], kbr.at[k, 0], partner)

    def kbrelay(k, i, mine):
        chip = (c - i + C) % C
        ref = kball.at[chip * 2 + (core if mine else 1 - core), k]
        return remote(ref, ref, krs.at[k, i], krr.at[k, i], partner)

    def sent(k):
        @pl.when(sec > 0)
        def _():
            for j in range(KH):
                usend(k, j).wait_send()

    def turn(k, carry):
        rows = pl.ds(pl.multiple_of(k * L, L), L)
        keys, values = [], []
        for j in range(KH):
            @pl.when(sec == S - 1)
            def _(j=j):
                cot_copy(k, j).wait()

            @pl.when(sec < S - 1)
            def _(j=j):
                usend(k, j).wait_recv()
            u = ubuf[k, j]
            us_ = jnp.concatenate(
                [u[:, g * HEAD_DIM:(g + 1) * HEAD_DIM] for g in range(G)], axis=0)
            key, q, pr = key_s[k, j], qst[k, j], prob[k, j]
            gp = dot_nt(us_, val_s[k, j])
            gv = dot_tn(pr.astype(BF16), us_).astype(BF16)
            rd = jnp.sum(pr * gp, axis=-1, keepdims=True)
            gs = (pr * (gp - rd) * scale).astype(BF16)
            gk = dot_tn(gs, q)
            gk = (gk * cos - pltpu.roll(gk, HEAD_DIM // 2, 1) * sin).astype(BF16)
            keys.append(gk)
            values.append(gv)
            kball[me, k, j] = jnp.concatenate([gk, gv], axis=1)
            gq = dot_nn(gs, key)
            for g in range(G):
                v = gq[g * L:(g + 1) * L]
                col = (j * G + g) * HEAD_DIM
                gnb[col // w, :, col % w:col % w + HEAD_DIM] = (
                    v * cos - pltpu.roll(v, HEAD_DIM // 2, 1) * sin)
            kbpartner(k, j).start()
            for i in range(1, C):
                kbcopy(k, j, i).start()
        @pl.when((sec == S - 1) & (k > 0))
        def _():
            sent(k - 1)
            pl.semaphore_signal(token, inc=1, device_id=(sec, partner), device_id_type=MESH)
        kbv = jnp.concatenate(keys + values, axis=1)
        part_inv = inv_s[rows, 0:1]
        proj = jnp.zeros((L, 1), F32)
        for d in range(N):
            gn = gnb[d] + dot_nt(kbv, wall[d])
            gnb[d] = gn
            gt = gn * x_ref[rows, d * w:(d + 1) * w].astype(F32) * part_inv
            proj = proj + jnp.sum(gt * gall[d][0:1, :], axis=-1, keepdims=True)
            gsh[d] += jnp.sum(gt.reshape(L // 8, 8, w), axis=0)
        proj = proj * (1.0 / D) * part_inv * part_inv
        @pl.when((sec == S - 1) & ((k > 0) | (core > 0)))
        def _():
            pl.semaphore_wait(token, 1)
        for j in range(KH):
            for e in range(N // KH):
                d = j * (N // KH) + e
                u = ubuf[k, j, :, e * w:(e + 1) * w].astype(F32)
                xd = x_ref[rows, d * w:(d + 1) * w].astype(F32)
                low = (u + part_inv * gall[d][0:1, :] * gnb[d] - xd * proj).astype(BF16)
                lowb[k, j, :, e * w:(e + 1) * w] = low
                low_out[rows, d * w:(d + 1) * w] = low

            @pl.when(sec > 0)
            def _(j=j):
                usend(k, j).start()
        return carry
    lax.fori_loop(0, B, turn, 0)

    @pl.when((sec == S - 1) & (core == 0))
    def _():
        sent(B - 1)
        pl.semaphore_signal(token, inc=1, device_id=(sec, partner), device_id_type=MESH)

    gsall[me] = gsh[me]
    for i in range(1, N):
        peer = (me + i) % N
        remote(gsh.at[peer], gsall.at[me], ssem.at[0], ssem.at[1], peer).start()
    for k in range(B):
        for i in range(1, C):
            chip = (c - i + C) % C
            wait_all(kball.at[chip * 2 + core, k], kbr.at[k, i])
            kbrelay(k, i, True).start()
    wait_all(nall.at[pl.ds(0, N - 1)], nsem.at[1])
    for k in range(B):
        wait_all(kball.at[partner, k], kbr.at[k, 0])
        for i in range(1, C):
            kbrelay(k, i, False).wait_recv()
    rows_all = nall[...].reshape(N * B * L, w)
    for j in range(KH):
        back = jnp.concatenate(
            [kball[g, k, j] for g in range(N) for k in range(B)], axis=0)
        dw = dot_tn(rows_all, back)
        gk_out[:, j * HEAD_DIM:(j + 1) * HEAD_DIM] = dw[:, :HEAD_DIM]
        gv_out[:, j * HEAD_DIM:(j + 1) * HEAD_DIM] = dw[:, HEAD_DIM:]
    wait_all(gsall.at[pl.ds(0, N - 1)], ssem.at[1])
    gg = gsall[0]
    for d in range(1, N):
        gg = gg + gsall[d]
    gg_out[...] = jnp.broadcast_to(jnp.sum(gg, axis=0, keepdims=True), gg_out.shape)

    wait_all(gall.at[pl.ds(0, N - 1)], gsem.at[0])
    wait_all(nall.at[pl.ds(0, N - 1)], nsem.at[0])
    wait_all(gsall.at[pl.ds(0, N - 1)], ssem.at[0])
    relayed(0, c, True, rls)
    for way in range(2):
        for t in range(C - 1):
            for p in range(PIECES):
                @pl.when(can_send(way, t) if p < OWN else can_send(way, t) & jnp.logical_not(upper))
                def _(way=way, t=t, p=p):
                    wcopy(way, t, p).wait_send()

            @pl.when(can_recv(way, t))
            def _(way=way, t=t):
                chip = c - 1 - t if way == 0 else c + 1 + t
                relayed(1 + way * (C - 1) + t, chip, True, rls)
            for p in range(OWN, PIECES):
                @pl.when(can_send(way, t) & jnp.logical_not(upper))
                def _(way=way, t=t, p=p):
                    hcopy(way, t, p).wait_send()

                @pl.when(can_recv(way, t) & jnp.logical_not(upper))
                def _(way=way, t=t, p=p):
                    hand(way, t, p).wait_send()
    for p in range(OWN, PIECES):
        @pl.when(upper)
        def _(p=p):
            to_pair(p).wait_send()
    for k in range(B):
        for i in range(C):
            wait_all(kball.at[me, k], kbs.at[k, i])
            if i:
                kbrelay(k, i, True).wait_send()

    @pl.when(sec < S - 1)
    def _():
        for k in range(B):
            sent(k)

    @pl.when((sec == S - 1) & (core == 1))
    def _():
        sent(B - 1)


def body(S, N, inputs, cotangent, norm_gain, key_weight, value_weight, plan):
    B, L, D = inputs.shape[1:]
    w, KV = key_weight.shape[1:]
    KH = KV // HEAD_DIM
    CW = D // KH
    G = CW // HEAD_DIM
    C = N // 2
    cos, sin = rope_tables(L)
    gain8 = jnp.broadcast_to(norm_gain.astype(F32), (8, w))
    vmem = pl.BlockSpec(memory_space=pltpu.VMEM)
    hbm = pl.BlockSpec(memory_space=pl.ANY)
    dma = pltpu.SemaphoreType.DMA
    low, gk, gv, gg = pl.pallas_call(
        functools.partial(kernel, S, N),
        out_shape=(
            jax.ShapeDtypeStruct((B * L, D), BF16),
            jax.ShapeDtypeStruct((w, KV), F32),
            jax.ShapeDtypeStruct((w, KV), F32),
            jax.ShapeDtypeStruct((8, w), F32),
        ),
        in_specs=[vmem, hbm, vmem, hbm, hbm, vmem, vmem],
        out_specs=(vmem,) * 4,
        scratch_shapes=[
            pltpu.VMEM((N, w, 2 * KV), BF16),
            pltpu.VMEM((N, B * L, w), BF16),
            pltpu.VMEM((N, B * L, w), BF16),
            pltpu.VMEM((N, 8, w), F32),
            pltpu.VMEM((B * L, 128), F32),
            pltpu.VMEM((B * L, 2 * KV), F32),
            pltpu.VMEM((B, KH, L, HEAD_DIM), BF16),
            pltpu.VMEM((B, KH, L, HEAD_DIM), BF16),
            pltpu.VMEM((B, KH, G * L, HEAD_DIM), BF16),
            pltpu.VMEM((B, KH, G * L, L), F32),
            pltpu.VMEM((B, KH, L, CW), BF16),
            pltpu.VMEM((B, KH, L, CW), BF16),
            pltpu.VMEM((N, L, w), F32),
            pltpu.VMEM((N, B, KH, L, 2 * HEAD_DIM), BF16),
            pltpu.VMEM((N, 8, w), F32),
            pltpu.VMEM((N, 8, w), F32),
            pltpu.VMEM((C, HELPED, w // PIECES, 2 * KV), BF16),
            dma((2,)),
            dma((2, C - 1, PIECES)),
            dma((2, C - 1, PIECES)),
            dma((2, C - 1, HELPED)),
            dma((2, C - 1, HELPED)),
            dma((2 * C - 1, HELPED)),
            dma((2 * C - 1, HELPED)),
            pltpu.SemaphoreType.REGULAR,
            dma((2 * C - 1,)),
            dma((2 * C - 1,)),
            dma((2,)),
            dma((2,)),
            dma((2,)),
            dma((B, KH)),
            dma((B, KH)),
            dma((B, KH)),
            dma((B, C)),
            dma((B, C)),
            dma((B, C)),
            dma((B, C)),
        ],
        compiler_params=pltpu.CompilerParams(
            collective_id=0, has_side_effects=True, vmem_limit_bytes=56 * 1024 * 1024),
    )(inputs[0].reshape(B * L, D), cotangent, gain8, key_weight[0], value_weight[0],
      jnp.asarray(cos), jnp.asarray(sin))
    low = low.reshape(B, L, D)
    selector = plan[0][:, None] == jnp.arange(B, dtype=jnp.int32)[None, :]
    ordered = jnp.sum(
        jnp.where(selector[:, :, None, None], low[None], jnp.zeros((), BF16)), axis=1)
    return ordered[None], gk[None], gv[None], gg[0:1]


def solution(mesh):
    in_specs = (
        P("section", None, "dp", None),
        P(None, "dp", None),
        P("section", "dp"),
        P("section", "dp", None),
        P("section", "dp", None),
        P("section", None),
    )
    out_specs = (
        P("section", None, "dp", None),
        P("section", "dp", None),
        P("section", "dp", None),
        P("section", "dp"),
    )
    run = functools.partial(body, mesh.shape["section"], mesh.shape["dp"])
    return jax.shard_map(run, mesh=mesh, in_specs=in_specs, out_specs=out_specs, check_vma=False)
```
